512 devices in a mesh: freq: 2 (over x_hi), base: 16 (over x_lo, y), pix: 16 (over z, core).
Axes of the slice: x: 4 (x_hi: 2, x_lo: 2; x = x_hi * 2 + x_lo), y: 8, z: 8, core: 2. Of those that a mesh axis runs over, the one named last changes fastest.
Arguments:
- sensing_operator_parts: bfloat16 [2, 16384, 32768], P('freq', 'base', 'pix'), may hold values from -1 to 1
- sampled_correlations: float32 [64, 16384], P('freq', 'base'), may hold values from -40 to 40
- first_sky_estimate: float32 [64, 16, 16, 128], P('freq', 'pix', 'base'), may hold values from -2.5 to 2.5
- patch_order_record: int32 [6, 256], P(None, 'pix'), may hold values from 0 to 255, as said below
Outputs:
- image: float32 [64, 16, 16, 128], P('freq', 'pix', 'base')
The draws below stay inside these ranges and needn't reach their ends.
Inputs may be any that keep to these rules, and one draw needn't show every extreme that they name: `patch_order_record`: each row holds every tile number once; the tiles of rank under 64 are the same in every row.
All inputs are finite; a program needn't handle non-finite values.
Results may differ from the reference program's by a relative error of at most 0.0014.
Values may be sent and summed in bfloat16 or wider, within the bound.
A program may use at most 64 MiB of HBM per device.

```python
import math
import jax
import jax.numpy as jnp
from jax import lax

CH = 64
TILE = 128
ITERS = 6
TILES_DEV = 1
GROUPS = 2
TSH = 128
NP = 32768
NM = 16384
NT = 256
KEEP = 64
N_BASE = 16
N_PIX = 16


def draw_sensing_operator_parts(key, part):
    key_base, key_tile, key_col = jax.random.split(jax.random.fold_in(key, 11), 3)
    tile_scaling = jnp.exp(jax.random.uniform(key_tile, (GROUPS, 1, NT, 1), jnp.float32, math.log(0.3), math.log(1.5)))
    col_scale = jax.random.uniform(key_col, (GROUPS, 1, NT, TILE), jnp.float32, 0.7, 1.3)
    scales = (tile_scaling * col_scale).reshape(GROUPS, 1, NP)
    values = jnp.clip(jax.random.normal(key_base, (GROUPS, NM, NP), jnp.float32), -4.0, 4.0)
    denom = math.sqrt(NM) + math.sqrt(NP)
    return jnp.clip(values * scales / denom, -1.0, 1.0).astype(jnp.bfloat16)


def draw_sampled_correlations(key, part):
    key_main = jax.random.fold_in(jax.random.fold_in(key, 23), 0)
    chan_scale = jnp.exp(math.log(3.0) * jnp.arange(CH, dtype=jnp.float32) / max(CH - 1, 1))
    values = jnp.clip(jax.random.normal(key_main, (CH, NM), jnp.float32), -5.0, 5.0)
    return jnp.clip(values * chan_scale[:, None], -40.0, 40.0)


def draw_patch_order_record(key, part):
    key_set, key_rows = jax.random.split(jax.random.fold_in(key, 37))
    tile_order = jax.random.permutation(key_set, NT).astype(jnp.int32)
    all_rows = []
    for iteration in range(ITERS):
        key_kept, key_rest = jax.random.split(jax.random.fold_in(key_rows, iteration))
        kept_rank = jax.random.permutation(key_kept, KEEP).astype(jnp.int32)
        rest_rank = (KEEP + jax.random.permutation(key_rest, NT - KEEP)).astype(jnp.int32)
        rank_values = jnp.concatenate([kept_rank, rest_rank])
        rank_row = jnp.zeros((NT,), jnp.int32).at[tile_order].set(rank_values)
        all_rows.append(rank_row)
    return jnp.stack(all_rows)


def steps_of(key, shape, pieces, least, largest):
    gain = 1.0
    for axis_at, shards_of in pieces:
        heights = jax.random.uniform(jax.random.fold_in(jax.random.fold_in(key, 6), axis_at), (shards_of,), jnp.float32, least / len(pieces), largest / len(pieces))
        gain = gain * jnp.repeat(jnp.exp(heights), shape[axis_at] // shards_of).reshape((-1,) + (1,) * (len(shape) - 1 - axis_at))
    return gain


def noise(own_key, extent, width, limit, cuts=(), kind=jnp.bfloat16):
    result = width * jax.random.normal(own_key, extent, jnp.float32)
    if cuts:
        result = result * steps_of(own_key, extent, cuts, -0.22, 0.18)
    return jnp.clip(result, -limit, limit).astype(kind)


def setup_inputs(seed: int = 0) -> dict:
    key_of = jax.random.split(jax.random.key(seed), 5)
    return {
        "sensing_operator_parts": draw_sensing_operator_parts(jax.random.fold_in(key_of[4], 71), 0),
        "sampled_correlations": draw_sampled_correlations(jax.random.fold_in(key_of[4], 71), 0),
        "first_sky_estimate": noise(key_of[2], (CH, N_PIX, N_BASE, TSH), 1.0, 2.5, ((0, 2), (1, 16), (2, 16)), jnp.float32),
        "patch_order_record": draw_patch_order_record(jax.random.fold_in(key_of[4], 71), 0),
    }


descent_stride = 0.6
lam_shrink = 0.3
eps_norm = 1e-06

def reference(sensing_operator_parts, sampled_correlations, first_sky_estimate, patch_order_record):
    chan_grp = CH // GROUPS
    current = first_sky_estimate.reshape(CH, NP)
    for step in range(ITERS):
        rounded_amount = current.astype(jnp.bfloat16)
        grads = []
        for spectral_band_set in range(GROUPS):
            sensing_operator = sensing_operator_parts[spectral_band_set]
            part = rounded_amount[spectral_band_set * chan_grp:(spectral_band_set + 1) * chan_grp]
            pred = lax.dot_general(part, sensing_operator, (((1,), (1,)), ((), ())), preferred_element_type=jnp.float32)
            resid = (sampled_correlations[spectral_band_set * chan_grp:(spectral_band_set + 1) * chan_grp] - pred).astype(jnp.bfloat16)
            grads.append(jnp.dot(resid, sensing_operator, preferred_element_type=jnp.float32))
        moved = current + descent_stride * jnp.concatenate(grads, axis=0)
        tiles = moved.reshape(CH, NT, TILE)
        tnorm = lax.optimization_barrier(jnp.sum(tiles * tiles, axis=(0, 2)))
        rms_tile = jnp.sqrt(tnorm / (CH * TILE) + eps_norm)
        keeping = (patch_order_record[step] < KEEP).astype(jnp.float32)
        factor = keeping * rms_tile / (rms_tile + lam_shrink)
        current = (tiles * factor[None, :, None]).reshape(CH, NP)
    return current.reshape(CH, N_PIX, N_BASE, TILES_DEV * TILE)
```

```python
import functools

import jax
import jax.numpy as jnp
from jax import lax
from jax.experimental import pallas as pl
from jax.experimental.pallas import tpu as pltpu
from jax.sharding import PartitionSpec as P

CH = 64
TILE = 128
ITERS = 6
STRIDE = 0.6
SHRINK = 0.3
EPS = 1e-06

F32 = jnp.float32
BF16 = jnp.bfloat16


def outward(n):
    out = [n // 2] if n > 1 else []
    for d in range((n - 1) // 2, 0, -1):
        out += [d, n - d]
    return out + [0]


def local_wait(ref, sem):
    pltpu.make_async_copy(ref, ref, sem).wait()


def kernel(
    nb, npx, keep_count,
    a_hbm, y_hbm, x0_hbm, rank_ref, out_ref,
    a_s, y_s, z_s, keep_s,
    zst, zrv, nst, nrv, acc, pst, prv, rst, rrv, gacc, gst, grv,
    in_sem, zs, zr, ns, nr, ps, pr, rs, rr, gs, gr,
):
    ny, nz = nb // 2, npx // 2
    f, b, p = lax.axis_index("freq"), lax.axis_index("base"), lax.axis_index("pix")
    xl, yy = b // ny, b % ny
    zz, cc = p // 2, p % 2
    rows = nz * TILE

    copy_x0 = pltpu.make_async_copy(x0_hbm, z_s, in_sem.at[0])
    copy_a = pltpu.make_async_copy(a_hbm, a_s, in_sem.at[1])
    copy_y = pltpu.make_async_copy(y_hbm, y_s, in_sem.at[2])
    copy_x0.start()
    copy_a.start()
    copy_y.start()

    base_peers = [((xl + dx) % 2 * ny + (yy + dy) % ny) for dy in outward(ny) for dx in (1, 0)]
    pix_peers = [((zz + dz) % nz, (cc + dc) % 2) for dz in outward(nz) for dc in (1, 0)]

    barrier = pltpu.get_barrier_semaphore()
    for other in base_peers:
        pl.semaphore_signal(barrier, 1, device_id={"freq": 1 - f, "base": other}, device_id_type=pl.DeviceIdType.MESH)
    for other in base_peers[:-1]:
        pl.semaphore_signal(barrier, 1, device_id={"base": other}, device_id_type=pl.DeviceIdType.MESH)
    for oz, oc in pix_peers[:-1]:
        pl.semaphore_signal(barrier, 1, device_id={"pix": oz * 2 + oc}, device_id_type=pl.DeviceIdType.MESH)

    same = lax.broadcasted_iota(jnp.int32, (nb, nb), 0) == lax.broadcasted_iota(jnp.int32, (nb, nb), 1)
    for k in range(ITERS):
        row = jnp.broadcast_to(rank_ref[k : k + 1, :], (nb, nb))
        column = jnp.sum(jnp.where(same & (row < keep_count), 1.0, 0.0), axis=1, keepdims=True)
        keep_s[k] = jnp.broadcast_to(column, (nb, TILE)).reshape(nb, 1, TILE)

    copy_x0.wait()
    copy_y.wait()
    pl.semaphore_wait(barrier, 2 * nb - 1 + npx - 1)
    copy_a.wait()

    def remote(src, dst, send, recv, where):
        return pltpu.make_async_remote_copy(
            src_ref=src, dst_ref=dst, send_sem=send, recv_sem=recv,
            device_id=where, device_id_type=pl.DeviceIdType.MESH,
        )

    def factor(k, tile):
        par = k % 2
        total = jnp.sum(nrv[par, 0, tile] + nrv[par, 1, tile], axis=1, keepdims=True)
        rms = jnp.sqrt(total / (CH * TILE) + EPS)
        value = keep_s[(k + ITERS - 1) % ITERS, tile] * (rms / (rms + SHRINK))
        return jnp.where(k == 0, 1.0, value)

    def norm_copies(k, to_all):
        par = k % 2
        out = []
        for i, other in enumerate(base_peers if to_all else [b]):
            out.append(remote(nst, nrv.at[par, f, b], ns.at[1, i], nr.at[par, f, b], {"freq": 1 - f, "base": other}))
        if to_all:
            for i, other in enumerate(base_peers[:-1]):
                out.append(remote(nst, nrv.at[par, f, b], ns.at[0, i], nr.at[par, f, b], {"base": other}))
        return out

    def put_norm(k, z):
        par = k % 2
        nst[...] = jnp.sum(z * z, axis=0, keepdims=True)
        return pltpu.make_async_copy(nst, nrv.at[par, f, b], nr.at[par, f, b])

    def step(k, carry):
        par = k % 2
        z = z_s[...]
        zst[...] = z.astype(BF16)
        own_norm = put_norm(k, z)
        own_z = pltpu.make_async_copy(zst, zrv.at[b], zr.at[b])
        n_sends = norm_copies(k, True)
        z_sends = [
            remote(zst, zrv.at[b], zs.at[i], zr.at[b], {"base": other})
            for i, other in enumerate(base_peers[:-1])
        ]
        own_z.start()
        own_norm.start()
        for c in n_sends:
            c.start()
        for c in z_sends:
            c.start()

        nq = ny // 2
        for i, dq in enumerate(reversed(outward(nq))):
            for dx in (0, 1):
                t0 = (xl + dx) % 2 * ny + (yy // 2 + dq) % nq * 2
                parts = []
                for t in (t0, t0 + 1):
                    local_wait(zrv.at[t], zr.at[t])
                    local_wait(nrv.at[par, 0, t], nr.at[par, 0, t])
                    local_wait(nrv.at[par, 1, t], nr.at[par, 1, t])
                    parts.append((zrv[t].astype(F32) * factor(k, t)).astype(BF16))
                lhs = jnp.concatenate(parts, axis=1)
                columns = pl.ds(pl.multiple_of(t0 * TILE, 2 * TILE), 2 * TILE)
                for n in range(0, rows, 256):
                    part = lax.dot_general(
                        lhs, a_s[n : n + 256, columns], (((1,), (1,)), ((), ())), preferred_element_type=F32
                    )
                    if i == 0 and dx == 0:
                        acc[:, n : n + 256] = part
                    else:
                        acc[:, n : n + 256] += part

        for z_ in range(nz):
            for c_ in range(2):
                pst[z_, c_] = acc[16 * c_ : 16 * c_ + 16, TILE * z_ : TILE * z_ + TILE].astype(BF16)
        p_sends = [
            remote(pst.at[oz, oc], prv.at[zz, cc], ps.at[i], pr.at[zz, cc], {"pix": oz * 2 + oc})
            for i, (oz, oc) in enumerate(pix_peers[:-1])
        ]
        for c in p_sends:
            c.start()
        total = pst[zz, cc].astype(F32)
        for oz, oc in reversed(pix_peers[:-1]):
            local_wait(prv.at[oz, oc], pr.at[oz, oc])
            total += prv[oz, oc].astype(F32)
        own_y = y_s[pl.ds(pl.multiple_of(cc * 16, 16), 16), pl.ds(pl.multiple_of(zz * TILE, TILE), TILE)]
        rst[...] = (own_y - total).astype(BF16)

        own_r = pltpu.make_async_copy(rst, rrv.at[zz, cc], rr.at[zz, cc])
        r_sends = [
            remote(rst, rrv.at[zz, cc], rs.at[i], rr.at[zz, cc], {"pix": oz * 2 + oc})
            for i, (oz, oc) in enumerate(pix_peers[:-1])
        ]
        own_r.start()
        for c in r_sends:
            c.start()
        nq = nz // 2
        for i, dq in enumerate(reversed(outward(nq))):
            z0 = (zz // 2 + dq) % nq * 2
            parts = []
            for z_ in (z0, z0 + 1):
                local_wait(rrv.at[z_, 0], rr.at[z_, 0])
                local_wait(rrv.at[z_, 1], rr.at[z_, 1])
                parts.append(jnp.concatenate([rrv[z_, 0], rrv[z_, 1]], axis=0))
            lhs = jnp.concatenate(parts, axis=1)
            these = pl.ds(pl.multiple_of(z0 * TILE, 2 * TILE), 2 * TILE)
            for n in range(nb // 2):
                part = jnp.dot(lhs, a_s[these, n * 256 : n * 256 + 256], preferred_element_type=F32)
                if i == 0:
                    gacc[n] = part
                else:
                    gacc[n] += part

        g_sends = [
            remote(gst.at[other], grv.at[b], gs.at[i], gr.at[b], {"base": other})
            for i, other in enumerate(base_peers[:-1])
        ]

        @pl.when(k > 0)
        def _():
            for c in g_sends:
                c.wait_send()

        for n in range(nb // 2):
            gst[2 * n] = gacc[n, :, :TILE].astype(BF16)
            gst[2 * n + 1] = gacc[n, :, TILE:].astype(BF16)
        for c in g_sends:
            c.start()
        for c in n_sends + z_sends + p_sends + r_sends:
            c.wait_send()
        x = z_s[...] * factor(k, b)
        total = gst[b].astype(F32)
        for other in reversed(base_peers[:-1]):
            local_wait(grv.at[other], gr.at[other])
            total += grv[other].astype(F32)
        z_s[...] = x + STRIDE * total
        return carry

    lax.fori_loop(0, ITERS, step, 0)

    for i, other in enumerate(base_peers[:-1]):
        remote(gst.at[other], grv.at[b], gs.at[i], gr.at[b], {"base": other}).wait_send()
    z = z_s[...]
    own_norm = put_norm(ITERS, z)
    (send,) = norm_copies(ITERS, False)
    send.start()
    own_norm.start()
    par = ITERS % 2
    for g in range(2):
        local_wait(nrv.at[par, g, b], nr.at[par, g, b])
    send.wait_send()
    out_ref[...] = z * factor(ITERS, b)


def on_device(nb, npx, sensing_operator_parts, sampled_correlations, first_sky_estimate, patch_order_record):
    a = sensing_operator_parts[0]
    chans, rows = sampled_correlations.shape
    pixels = a.shape[1]
    nz = npx // 2
    dma = pltpu.SemaphoreType.DMA
    anywhere = pl.BlockSpec(memory_space=pl.ANY)
    vmem = pl.BlockSpec(memory_space=pltpu.VMEM)
    image = pl.pallas_call(
        functools.partial(kernel, nb, npx, nb * npx // 4),
        out_shape=jax.ShapeDtypeStruct((chans, TILE), F32),
        in_specs=[anywhere, anywhere, anywhere, vmem],
        out_specs=vmem,
        scratch_shapes=[
            pltpu.VMEM((rows, pixels), BF16),
            pltpu.VMEM((chans, rows), F32),
            pltpu.VMEM((chans, TILE), F32),
            pltpu.VMEM((ITERS, nb, 1, TILE), F32),
            pltpu.VMEM((chans, TILE), BF16),
            pltpu.VMEM((nb, chans, TILE), BF16),
            pltpu.VMEM((1, TILE), F32),
            pltpu.VMEM((2, 2, nb, 1, TILE), F32),
            pltpu.VMEM((chans, rows), F32),
            pltpu.VMEM((nz, 2, 16, TILE), BF16),
            pltpu.VMEM((nz, 2, 16, TILE), BF16),
            pltpu.VMEM((16, TILE), BF16),
            pltpu.VMEM((nz, 2, 16, TILE), BF16),
            pltpu.VMEM((nb // 2, chans, 2 * TILE), F32),
            pltpu.VMEM((nb, chans, TILE), BF16),
            pltpu.VMEM((nb, chans, TILE), BF16),
            dma((3,)),
            dma((nb,)), dma((nb,)),
            dma((2, nb)), dma((2, 2, nb)),
            dma((npx,)), dma((nz, 2)),
            dma((npx,)), dma((nz, 2)),
            dma((nb,)), dma((nb,)),
        ],
        compiler_params=pltpu.CompilerParams(collective_id=0, has_side_effects=True),
        name="shrinkage",
    )(a, sampled_correlations, first_sky_estimate.reshape(chans, TILE), patch_order_record)
    return image.reshape(chans, 1, 1, TILE)


def solution(mesh):
    in_specs = (
        P("freq", "base", "pix"),
        P("freq", "base"),
        P("freq", "pix", "base", None),
        P(None, "pix"),
    )
    out_specs = P("freq", "pix", "base", None)
    return jax.shard_map(
        functools.partial(on_device, mesh.shape["base"], mesh.shape["pix"]),
        mesh=mesh, in_specs=in_specs, out_specs=out_specs, check_vma=False,
    )
```

```python
import functools

import jax
import jax.numpy as jnp
from jax import lax
from jax.experimental import pallas as pl
from jax.experimental.pallas import tpu as pltpu
from jax.sharding import PartitionSpec as P

CH = 64
TILE = 128
ITERS = 6
STRIDE = 0.6
SHRINK = 0.3
EPS = 1e-06
OWNER = 1

F32 = jnp.float32
BF16 = jnp.bfloat16


def outward(n):
    out = [n // 2] if n > 1 else []
    for d in range((n - 1) // 2, 0, -1):
        out += [d, n - d]
    return out + [0]


def local_wait(ref, sem):
    pltpu.make_async_copy(ref, ref, sem).wait()


def kernel(
    nb, npx, keep_count,
    a_hbm, y_hbm, x0_hbm, rank_ref, out_ref,
    a_s, at_s, y_s, z_s, keep_s,
    zrv, nst, nrv, acc, pst, prv, rrv, gacc, gst, grv,
    in_sem, zs, zr, ns, nr, ps, pr, rs, rr, gs, gr,
):
    ny, nz = nb // 2, npx // 2
    nq_y = ny // 2
    f, b, p = lax.axis_index("freq"), lax.axis_index("base"), lax.axis_index("pix")
    xl, yy = b // ny, b % ny
    zz, cc = p // 2, p % 2
    rows = nz * TILE

    copy_x0 = pltpu.make_async_copy(x0_hbm, z_s, in_sem.at[0])
    copy_a = pltpu.make_async_copy(a_hbm, a_s, in_sem.at[1])
    copy_y = pltpu.make_async_copy(y_hbm, y_s, in_sem.at[2])
    copy_x0.start()
    copy_a.start()
    copy_y.start()

    base_peers = [((xl + dx) % 2 * ny + (yy + dy) % ny) for dy in outward(ny) for dx in (1, 0)]
    pix_peers = [((zz + dz) % nz, (cc + dc) % 2) for dz in outward(nz) for dc in (1, 0)]

    barrier = pltpu.get_barrier_semaphore()
    for other in base_peers:
        pl.semaphore_signal(barrier, 1, device_id={"freq": 1 - f, "base": other}, device_id_type=pl.DeviceIdType.MESH)
    for other in base_peers[:-1]:
        pl.semaphore_signal(barrier, 1, device_id={"base": other}, device_id_type=pl.DeviceIdType.MESH)
    for oz, oc in pix_peers[:-1]:
        pl.semaphore_signal(barrier, 1, device_id={"pix": oz * 2 + oc}, device_id_type=pl.DeviceIdType.MESH)

    same = lax.broadcasted_iota(jnp.int32, (nb, nb), 0) == lax.broadcasted_iota(jnp.int32, (nb, nb), 1)
    for k in range(ITERS):
        row = jnp.broadcast_to(rank_ref[k : k + 1, :], (nb, nb))
        column = jnp.sum(jnp.where(same & (row < keep_count), 1.0, 0.0), axis=1, keepdims=True)
        keep_s[k] = jnp.broadcast_to(column, (nb, TILE)).reshape(nb, 1, TILE)

    copy_x0.wait()
    copy_y.wait()
    pl.semaphore_wait(barrier, 2 * nb - 1 + npx - 1)

    def remote(src, dst, send, recv, where):
        return pltpu.make_async_remote_copy(
            src_ref=src, dst_ref=dst, send_sem=send, recv_sem=recv,
            device_id=where, device_id_type=pl.DeviceIdType.MESH,
        )

    def norm_of(z):
        return jnp.sum(z * z, axis=0, keepdims=True)

    def factor(k, tile, own_norm):
        total = jnp.sum(own_norm + nrv[k % 2, tile], axis=1, keepdims=True)
        rms = jnp.sqrt(total / (CH * TILE) + EPS)
        value = keep_s[(k + ITERS - 1) % ITERS, tile] * (rms / (rms + SHRINK))
        return jnp.where(k == 0, 1.0, value)

    def norm_copies(k, to):
        return [
            remote(nst, nrv.at[k % 2, b], ns.at[i], nr.at[k % 2, b], {"freq": 1 - f, "base": other})
            for i, other in enumerate(to)
        ]

    def step(k, carry):
        par = k % 2
        rounded = z_s[...].astype(BF16)
        zrv[b] = rounded
        nst[...] = norm_of(rounded.astype(F32))
        n_sends = norm_copies(k, base_peers)
        z_sends = [
            remote(zrv.at[b], zrv.at[b], zs.at[i], zr.at[b], {"base": other})
            for i, other in enumerate(base_peers[:-1])
        ]
        for c in n_sends + z_sends:
            c.start()

        @pl.when(k == 0)
        def _():
            copy_a.wait()

            def turn(j, carry):
                block = pl.ds(pl.multiple_of(j * TILE, TILE), TILE)
                at_s[block, :] = a_s[:, block].T
                return carry

            lax.fori_loop(0, nb, turn, 0)

        for i, dq in enumerate(reversed(outward(nq_y))):
            y0 = (yy // 2 + dq) % nq_y * 2
            firsts = [xl * ny + y0, (1 - xl) * ny + y0]
            arrive = [firsts[0], firsts[0] + 1, firsts[1], firsts[1] + 1]
            if dq == 0:
                arrive = [firsts[0] + 1 - yy % 2, firsts[1], firsts[1] + 1]
            for t in arrive:
                local_wait(zrv.at[t], zr.at[t])
            for t0 in firsts:
                for t in (t0, t0 + 1):
                    local_wait(nrv.at[par, t], nr.at[par, t])
            for t0 in firsts:
                parts = []
                for t in (t0, t0 + 1):
                    tile = zrv[t].astype(F32)
                    parts.append((tile * factor(k, t, norm_of(tile))).astype(BF16))
                lhs = jnp.concatenate(parts, axis=1)
                these = pl.ds(pl.multiple_of(t0 * TILE, 2 * TILE), 2 * TILE)
                for n in range(0, rows, 256):
                    part = jnp.dot(lhs, at_s[these, n : n + 256], preferred_element_type=F32)
                    if i == 0 and t0 is firsts[0]:
                        acc[:, n : n + 256] = part
                    else:
                        acc[:, n : n + 256] += part

        half = nz // 2
        for z_ in range(nz):
            pst[z_ % half, z_ // half] = acc[:, TILE * z_ : TILE * z_ + TILE].astype(BF16)
        p_sends = [
            remote(
                pst.at[(zz + dz) % nz % half], prv.at[par, zz, cc], ps.at[i], pr.at[par, zz, cc],
                {"pix": (zz + dz) % nz * 2 + OWNER},
            )
            for i, dz in enumerate(outward(nz))
        ]
        for c in p_sends[:-1]:
            c.start()
        mine = zz % half
        near = [0]
        for d in range(1, half // 2 + 1):
            near += [d] if 2 * d == half else [d, -d]
        r_sends = [
            remote(rrv.at[mine], rrv.at[mine], rs.at[i], rr.at[mine], {"pix": (zz + d + nz) % nz * 2 + c_})
            for i, (d, c_) in enumerate((d, c_) for d in reversed(near) for c_ in (1 - OWNER, OWNER))
        ][:-1]

        @pl.when(cc != OWNER)
        def _():
            p_sends[-1].start()
            local_wait(rrv.at[mine], rr.at[mine])

        @pl.when(cc == OWNER)
        def _():
            total = pst[mine].astype(F32)
            for dz in reversed(outward(nz)):
                oz = (zz + dz) % nz
                for c_ in (0, 1):
                    if (dz, c_) != (0, OWNER):
                        local_wait(prv.at[par, oz, c_], pr.at[par, oz, c_])
                        total += prv[par, oz, c_].astype(F32)
            for h in range(2):
                own_y = y_s[:, pl.ds(pl.multiple_of((mine + h * half) * TILE, TILE), TILE)]
                rrv[mine, h] = (own_y - total[h]).astype(BF16)
            for c in r_sends:
                c.start()

        for i, d in enumerate(near):
            q = (zz - d + nz) % half
            if d != 0:
                local_wait(rrv.at[q], rr.at[q])
            lhs = jnp.concatenate([rrv[q, 0], rrv[q, 1]], axis=1)
            low = pl.ds(pl.multiple_of(q * TILE, TILE), TILE)
            high = pl.ds(pl.multiple_of((q + half) * TILE, TILE), TILE)
            if i < len(near) - 1:
                for n in range(nb // 2):
                    cols = slice(n * 256, n * 256 + 256)
                    rhs = jnp.concatenate([a_s[low, cols], a_s[high, cols]], axis=0)
                    part = jnp.dot(lhs, rhs, preferred_element_type=F32)
                    if i == 0:
                        gacc[n] = part
                    else:
                        gacc[n] += part

        def g_copy(i, other):
            return remote(gst.at[other], grv.at[b], gs.at[i], gr.at[b], {"base": other})

        g_pairs = [((xl + dx) % 2 * ny + (yy // 2 + dq) % nq_y * 2) for dq in outward(nq_y) for dx in (1, 0)]
        g_order = []
        for t0 in g_pairs[:-1]:
            g_order += [t0, t0 + 1]
        g_order.append(g_pairs[-1] + 1 - yy % 2)
        g_sends = [g_copy(i, other) for i, other in enumerate(g_order)]

        @pl.when(k > 0)
        def _():
            for c in g_sends:
                c.wait_send()

        batch = max(len(g_pairs) // 2, 1)
        for j in range(0, len(g_pairs), batch):
            for t0 in g_pairs[j : j + batch]:
                cols = pl.ds(pl.multiple_of(t0 * TILE, 2 * TILE), 2 * TILE)
                rhs = jnp.concatenate([a_s[low, cols], a_s[high, cols]], axis=0)
                part = jnp.dot(lhs, rhs, preferred_element_type=F32)
                if len(near) > 1:
                    part += gacc[t0 // 2]
                gst[t0] = part[:, :TILE].astype(BF16)
                gst[t0 + 1] = part[:, TILE:].astype(BF16)
            for c in g_sends[2 * j : 2 * (j + batch)]:
                c.start()
        for c in n_sends + z_sends + p_sends[:-1]:
            c.wait_send()

        @pl.when(cc != OWNER)
        def _():
            p_sends[-1].wait_send()

        @pl.when(cc == OWNER)
        def _():
            for c in r_sends:
                c.wait_send()

        x = z_s[...] * factor(k, b, norm_of(zrv[b].astype(F32)))
        total = gst[b].astype(F32)
        for other in reversed(base_peers[:-1]):
            local_wait(grv.at[other], gr.at[other])
            total += grv[other].astype(F32)
        z_s[...] = x + STRIDE * total
        return carry

    lax.fori_loop(0, ITERS, step, 0)

    for i, other in enumerate(base_peers[:-1]):
        remote(gst.at[other], grv.at[b], gs.at[i], gr.at[b], {"base": other}).wait_send()
    z = z_s[...]
    nst[...] = norm_of(z)
    (send,) = norm_copies(ITERS, [b])
    send.start()
    local_wait(nrv.at[ITERS % 2, b], nr.at[ITERS % 2, b])
    send.wait_send()
    out_ref[...] = z * factor(ITERS, b, nst[...])


def on_device(nb, npx, sensing_operator_parts, sampled_correlations, first_sky_estimate, patch_order_record):
    a = sensing_operator_parts[0]
    chans, rows = sampled_correlations.shape
    pixels = a.shape[1]
    nz = npx // 2
    dma = pltpu.SemaphoreType.DMA
    anywhere = pl.BlockSpec(memory_space=pl.ANY)
    vmem = pl.BlockSpec(memory_space=pltpu.VMEM)
    image = pl.pallas_call(
        functools.partial(kernel, nb, npx, nb * npx // 4),
        out_shape=jax.ShapeDtypeStruct((chans, TILE), F32),
        in_specs=[anywhere, anywhere, anywhere, vmem],
        out_specs=vmem,
        scratch_shapes=[
            pltpu.VMEM((rows, pixels), BF16),
            pltpu.VMEM((pixels, rows), BF16),
            pltpu.VMEM((chans, rows), F32),
            pltpu.VMEM((chans, TILE), F32),
            pltpu.VMEM((ITERS, nb, 1, TILE), F32),
            pltpu.VMEM((nb, chans, TILE), BF16),
            pltpu.VMEM((1, TILE), F32),
            pltpu.VMEM((2, nb, 1, TILE), F32),
            pltpu.VMEM((chans, rows), F32),
            pltpu.VMEM((nz // 2, 2, chans, TILE), BF16),
            pltpu.VMEM((2, nz, 2, 2, chans, TILE), BF16),
            pltpu.VMEM((nz // 2, 2, chans, TILE), BF16),
            pltpu.VMEM((nb // 2, chans, 2 * TILE), F32),
            pltpu.VMEM((nb, chans, TILE), BF16),
            pltpu.VMEM((nb, chans, TILE), BF16),
            dma((3,)),
            dma((nb,)), dma((nb,)),
            dma((nb,)), dma((2, nb)),
            dma((nz,)), dma((2, nz, 2)),
            dma((nz,)), dma((nz // 2,)),
            dma((nb,)), dma((nb,)),
        ],
        compiler_params=pltpu.CompilerParams(collective_id=0, has_side_effects=True),
        name="shrinkage",
    )(a, sampled_correlations, first_sky_estimate.reshape(chans, TILE), patch_order_record)
    return image.reshape(chans, 1, 1, TILE)


def solution(mesh):
    in_specs = (
        P("freq", "base", "pix"),
        P("freq", "base"),
        P("freq", "pix", "base", None),
        P(None, "pix"),
    )
    out_specs = P("freq", "pix", "base", None)
    return jax.shard_map(
        functools.partial(on_device, mesh.shape["base"], mesh.shape["pix"]),
        mesh=mesh, in_specs=in_specs, out_specs=out_specs, check_vma=False,
    )
```

```python
import functools

import jax
import jax.numpy as jnp
from jax import lax
from jax.experimental import pallas as pl
from jax.experimental.pallas import tpu as pltpu
from jax.sharding import PartitionSpec as P

CH = 64
TILE = 128
ITERS = 6
STRIDE = 0.6
SHRINK = 0.3
EPS = 1e-06
OWNER = 1

F32 = jnp.float32
BF16 = jnp.bfloat16


def outward(n):
    out = [n // 2] if n > 1 else []
    for d in range((n - 1) // 2, 0, -1):
        out += [d, n - d]
    return out + [0]


def local_wait(ref, sem):
    pltpu.make_async_copy(ref, ref, sem).wait()


def kernel(
    nb, npx, keep_count,
    a_hbm, y_hbm, x0_hbm, rank_ref, out_ref,
    a_s, at_s, y_s, z_s, keep_s,
    zrv, nst, nrv, acc, pst, psent, ptot, prv, rrv, gacc, gst, gsent, gtot, grv,
    in_sem, zs, zr, ns, nr, ps, pr, rs, rr, gs, gr,
):
    ny, nz = nb // 2, npx // 2
    nq_y = ny // 2
    f, b, p = lax.axis_index("freq"), lax.axis_index("base"), lax.axis_index("pix")
    xl, yy = b // ny, b % ny
    zz, cc = p // 2, p % 2
    rows = nz * TILE

    copy_x0 = pltpu.make_async_copy(x0_hbm, z_s, in_sem.at[0])
    copy_a = pltpu.make_async_copy(a_hbm, a_s, in_sem.at[1])
    copy_y = pltpu.make_async_copy(y_hbm, y_s, in_sem.at[2])
    copy_x0.start()
    copy_a.start()
    copy_y.start()

    base_peers = [((xl + dx) % 2 * ny + (yy + dy) % ny) for dy in outward(ny) for dx in (1, 0)]
    pix_peers = [((zz + dz) % nz, (cc + dc) % 2) for dz in outward(nz) for dc in (1, 0)]

    barrier = pltpu.get_barrier_semaphore()
    for other in base_peers:
        pl.semaphore_signal(barrier, 1, device_id={"freq": 1 - f, "base": other}, device_id_type=pl.DeviceIdType.MESH)
    for other in base_peers[:-1]:
        pl.semaphore_signal(barrier, 1, device_id={"base": other}, device_id_type=pl.DeviceIdType.MESH)
    for oz, oc in pix_peers[:-1]:
        pl.semaphore_signal(barrier, 1, device_id={"pix": oz * 2 + oc}, device_id_type=pl.DeviceIdType.MESH)

    same = lax.broadcasted_iota(jnp.int32, (nb, nb), 0) == lax.broadcasted_iota(jnp.int32, (nb, nb), 1)
    for k in range(ITERS):
        row = jnp.broadcast_to(rank_ref[k : k + 1, :], (nb, nb))
        column = jnp.sum(jnp.where(same & (row < keep_count), 1.0, 0.0), axis=1, keepdims=True)
        keep_s[k] = jnp.broadcast_to(column, (nb, TILE)).reshape(nb, 1, TILE)

    for ref in (psent, ptot, gsent, gtot):
        ref[...] = jnp.zeros_like(ref)

    copy_x0.wait()
    copy_y.wait()
    pl.semaphore_wait(barrier, 2 * nb - 1 + npx - 1)

    def remote(src, dst, send, recv, where):
        return pltpu.make_async_remote_copy(
            src_ref=src, dst_ref=dst, send_sem=send, recv_sem=recv,
            device_id=where, device_id_type=pl.DeviceIdType.MESH,
        )

    def norm_of(z):
        return jnp.sum(z * z, axis=0, keepdims=True)

    def factor(k, tile, own_norm):
        total = jnp.sum(own_norm + nrv[k % 2, tile], axis=1, keepdims=True)
        rms = jnp.sqrt(total / (CH * TILE) + EPS)
        value = keep_s[(k + ITERS - 1) % ITERS, tile] * (rms / (rms + SHRINK))
        return jnp.where(k == 0, 1.0, value)

    def norm_copies(k, to):
        return [
            remote(nst, nrv.at[k % 2, b], ns.at[i], nr.at[k % 2, b], {"freq": 1 - f, "base": other})
            for i, other in enumerate(to)
        ]

    def step(k, carry):
        par = k % 2
        rounded = z_s[...].astype(BF16)
        zrv[b] = rounded
        nst[...] = norm_of(rounded.astype(F32))
        n_sends = norm_copies(k, base_peers)
        z_sends = [
            remote(zrv.at[b], zrv.at[b], zs.at[i], zr.at[b], {"base": other})
            for i, other in enumerate(base_peers[:-1])
        ]
        for c in n_sends + z_sends:
            c.start()

        @pl.when(k == 0)
        def _():
            copy_a.wait()

            def turn(j, carry):
                block = pl.ds(pl.multiple_of(j * TILE, TILE), TILE)
                at_s[block, :] = a_s[:, block].T
                return carry

            lax.fori_loop(0, nb, turn, 0)

        for i, dq in enumerate(reversed(outward(nq_y))):
            y0 = (yy // 2 + dq) % nq_y * 2
            firsts = [xl * ny + y0, (1 - xl) * ny + y0]
            arrive = [firsts[0], firsts[0] + 1, firsts[1], firsts[1] + 1]
            if dq == 0:
                arrive = [firsts[0] + 1 - yy % 2, firsts[1], firsts[1] + 1]
            for t in arrive:
                local_wait(zrv.at[t], zr.at[t])
            for t0 in firsts:
                for t in (t0, t0 + 1):
                    local_wait(nrv.at[par, t], nr.at[par, t])
            for t0 in firsts:
                parts = []
                for t in (t0, t0 + 1):
                    tile = zrv[t].astype(F32)
                    parts.append((tile * factor(k, t, norm_of(tile))).astype(BF16))
                lhs = jnp.concatenate(parts, axis=1)
                these = pl.ds(pl.multiple_of(t0 * TILE, 2 * TILE), 2 * TILE)
                for n in range(0, rows, 256):
                    part = jnp.dot(lhs, at_s[these, n : n + 256], preferred_element_type=F32)
                    if i == 0 and t0 is firsts[0]:
                        acc[:, n : n + 256] = part
                    else:
                        acc[:, n : n + 256] += part

        half = nz // 2
        for z_ in range(nz):
            at = z_ % half, z_ // half
            pst[at] = (acc[:, TILE * z_ : TILE * z_ + TILE] - psent[at]).astype(BF16)
        p_sends = [
            remote(
                pst.at[(zz + dz) % nz % half], prv.at[par, zz, cc], ps.at[i], pr.at[par, zz, cc],
                {"pix": (zz + dz) % nz * 2 + OWNER},
            )
            for i, dz in enumerate(outward(nz))
        ]
        for c in p_sends[:-1]:
            c.start()
        psent[...] += pst[...].astype(F32)
        mine = zz % half
        near = [0]
        for d in range(1, half // 2 + 1):
            near += [d] if 2 * d == half else [d, -d]
        r_sends = [
            remote(rrv.at[mine], rrv.at[mine], rs.at[i], rr.at[mine], {"pix": (zz + d + nz) % nz * 2 + c_})
            for i, (d, c_) in enumerate((d, c_) for d in reversed(near) for c_ in (1 - OWNER, OWNER))
        ][:-1]

        @pl.when(cc != OWNER)
        def _():
            p_sends[-1].start()
            local_wait(rrv.at[mine], rr.at[mine])

        @pl.when(cc == OWNER)
        def _():
            total = ptot[...] + pst[mine].astype(F32)
            for dz in reversed(outward(nz)):
                oz = (zz + dz) % nz
                for c_ in (0, 1):
                    if (dz, c_) != (0, OWNER):
                        local_wait(prv.at[par, oz, c_], pr.at[par, oz, c_])
                        total += prv[par, oz, c_].astype(F32)
            ptot[...] = total
            for h in range(2):
                own_y = y_s[:, pl.ds(pl.multiple_of((mine + h * half) * TILE, TILE), TILE)]
                rrv[mine, h] = (own_y - total[h]).astype(BF16)
            for c in r_sends:
                c.start()

        for i, d in enumerate(near):
            q = (zz - d + nz) % half
            if d != 0:
                local_wait(rrv.at[q], rr.at[q])
            lhs = jnp.concatenate([rrv[q, 0], rrv[q, 1]], axis=1)
            low = pl.ds(pl.multiple_of(q * TILE, TILE), TILE)
            high = pl.ds(pl.multiple_of((q + half) * TILE, TILE), TILE)
            if i < len(near) - 1:
                for n in range(nb // 2):
                    cols = slice(n * 256, n * 256 + 256)
                    rhs = jnp.concatenate([a_s[low, cols], a_s[high, cols]], axis=0)
                    part = jnp.dot(lhs, rhs, preferred_element_type=F32)
                    if i == 0:
                        gacc[n] = part
                    else:
                        gacc[n] += part

        def g_copy(i, other):
            return remote(gst.at[other], grv.at[b], gs.at[i], gr.at[b], {"base": other})

        g_pairs = [((xl + dx) % 2 * ny + (yy // 2 + dq) % nq_y * 2) for dq in outward(nq_y) for dx in (1, 0)]
        g_order = []
        for t0 in g_pairs[:-1]:
            g_order += [t0, t0 + 1]
        g_order.append(g_pairs[-1] + 1 - yy % 2)
        g_sends = [g_copy(i, other) for i, other in enumerate(g_order)]

        @pl.when(k > 0)
        def _():
            for c in g_sends:
                c.wait_send()

        batch = max(len(g_pairs) // 2, 1)
        for j in range(0, len(g_pairs), batch):
            for t0 in g_pairs[j : j + batch]:
                cols = pl.ds(pl.multiple_of(t0 * TILE, 2 * TILE), 2 * TILE)
                rhs = jnp.concatenate([a_s[low, cols], a_s[high, cols]], axis=0)
                part = jnp.dot(lhs, rhs, preferred_element_type=F32)
                if len(near) > 1:
                    part += gacc[t0 // 2]
                gst[t0] = (part[:, :TILE] - gsent[t0]).astype(BF16)
                gst[t0 + 1] = (part[:, TILE:] - gsent[t0 + 1]).astype(BF16)
            for c in g_sends[2 * j : 2 * (j + batch)]:
                c.start()
        for c in n_sends + z_sends + p_sends[:-1]:
            c.wait_send()

        @pl.when(cc != OWNER)
        def _():
            p_sends[-1].wait_send()

        @pl.when(cc == OWNER)
        def _():
            for c in r_sends:
                c.wait_send()

        gsent[...] += gst[...].astype(F32)
        x = z_s[...] * factor(k, b, norm_of(zrv[b].astype(F32)))
        total = gtot[...] + gst[b].astype(F32)
        for other in reversed(base_peers[:-1]):
            local_wait(grv.at[other], gr.at[other])
            total += grv[other].astype(F32)
        gtot[...] = total
        z_s[...] = x + STRIDE * total
        return carry

    lax.fori_loop(0, ITERS, step, 0)

    for i, other in enumerate(base_peers[:-1]):
        remote(gst.at[other], grv.at[b], gs.at[i], gr.at[b], {"base": other}).wait_send()
    z = z_s[...]
    nst[...] = norm_of(z)
    (send,) = norm_copies(ITERS, [b])
    send.start()
    local_wait(nrv.at[ITERS % 2, b], nr.at[ITERS % 2, b])
    send.wait_send()
    out_ref[...] = z * factor(ITERS, b, nst[...])


def on_device(nb, npx, sensing_operator_parts, sampled_correlations, first_sky_estimate, patch_order_record):
    a = sensing_operator_parts[0]
    chans, rows = sampled_correlations.shape
    pixels = a.shape[1]
    nz = npx // 2
    dma = pltpu.SemaphoreType.DMA
    anywhere = pl.BlockSpec(memory_space=pl.ANY)
    vmem = pl.BlockSpec(memory_space=pltpu.VMEM)
    image = pl.pallas_call(
        functools.partial(kernel, nb, npx, nb * npx // 4),
        out_shape=jax.ShapeDtypeStruct((chans, TILE), F32),
        in_specs=[anywhere, anywhere, anywhere, vmem],
        out_specs=vmem,
        scratch_shapes=[
            pltpu.VMEM((rows, pixels), BF16),
            pltpu.VMEM((pixels, rows), BF16),
            pltpu.VMEM((chans, rows), F32),
            pltpu.VMEM((chans, TILE), F32),
            pltpu.VMEM((ITERS, nb, 1, TILE), F32),
            pltpu.VMEM((nb, chans, TILE), BF16),
            pltpu.VMEM((1, TILE), F32),
            pltpu.VMEM((2, nb, 1, TILE), F32),
            pltpu.VMEM((chans, rows), F32),
            pltpu.VMEM((nz // 2, 2, chans, TILE), BF16),
            pltpu.VMEM((nz // 2, 2, chans, TILE), F32),
            pltpu.VMEM((2, chans, TILE), F32),
            pltpu.VMEM((2, nz, 2, 2, chans, TILE), BF16),
            pltpu.VMEM((nz // 2, 2, chans, TILE), BF16),
            pltpu.VMEM((nb // 2, chans, 2 * TILE), F32),
            pltpu.VMEM((nb, chans, TILE), BF16),
            pltpu.VMEM((nb, chans, TILE), F32),
            pltpu.VMEM((chans, TILE), F32),
            pltpu.VMEM((nb, chans, TILE), BF16),
            dma((3,)),
            dma((nb,)), dma((nb,)),
            dma((nb,)), dma((2, nb)),
            dma((nz,)), dma((2, nz, 2)),
            dma((nz,)), dma((nz // 2,)),
            dma((nb,)), dma((nb,)),
        ],
        compiler_params=pltpu.CompilerParams(collective_id=0, has_side_effects=True),
        name="shrinkage",
    )(a, sampled_correlations, first_sky_estimate.reshape(chans, TILE), patch_order_record)
    return image.reshape(chans, 1, 1, TILE)


def solution(mesh):
    in_specs = (
        P("freq", "base", "pix"),
        P("freq", "base"),
        P("freq", "pix", "base", None),
        P(None, "pix"),
    )
    out_specs = P("freq", "pix", "base", None)
    return jax.shard_map(
        functools.partial(on_device, mesh.shape["base"], mesh.shape["pix"]),
        mesh=mesh, in_specs=in_specs, out_specs=out_specs, check_vma=False,
    )
```

```python
import functools

import jax
import jax.numpy as jnp
from jax import lax
from jax.experimental import pallas as pl
from jax.experimental.pallas import tpu as pltpu
from jax.sharding import PartitionSpec as P

CH = 64
TILE = 128
ITERS = 6
STRIDE = 0.6
SHRINK = 0.3
EPS = 1e-06
OWNER = 1

F32 = jnp.float32
BF16 = jnp.bfloat16


def outward(n):
    out = [n // 2] if n > 1 else []
    for d in range((n - 1) // 2, 0, -1):
        out += [d, n - d]
    return out + [0]


def local_wait(ref, sem):
    pltpu.make_async_copy(ref, ref, sem).wait()


def kernel(
    nb, npx, keep_count,
    a_hbm, y_hbm, x0_hbm, rank_ref, out_ref,
    a_s, at_s, y_s, z_s, keep_s,
    zrv, nst, nrv, acc, pst, psent, ptot, prv, rrv, gacc, gst, gsent, gtot, grv,
    in_sem, zs, zr, ns, nr, ps, pr, rs, rr, gs, gr,
):
    ny, nz = nb // 2, npx // 2
    nq_y = ny // 2
    f, b, p = lax.axis_index("freq"), lax.axis_index("base"), lax.axis_index("pix")
    xl, yy = b // ny, b % ny
    zz, cc = p // 2, p % 2
    rows = nz * TILE

    copy_x0 = pltpu.make_async_copy(x0_hbm, z_s, in_sem.at[0])
    copy_a = pltpu.make_async_copy(a_hbm, a_s, in_sem.at[1])
    copy_y = pltpu.make_async_copy(y_hbm, y_s, in_sem.at[2])
    copy_x0.start()
    copy_a.start()
    copy_y.start()

    base_peers = [((xl + dx) % 2 * ny + (yy + dy) % ny) for dy in outward(ny) for dx in (1, 0)]
    pix_peers = [((zz + dz) % nz, (cc + dc) % 2) for dz in outward(nz) for dc in (1, 0)]

    barrier = pltpu.get_barrier_semaphore()
    for other in base_peers:
        pl.semaphore_signal(barrier, 1, device_id={"freq": 1 - f, "base": other}, device_id_type=pl.DeviceIdType.MESH)
    for other in base_peers[:-1]:
        pl.semaphore_signal(barrier, 1, device_id={"base": other}, device_id_type=pl.DeviceIdType.MESH)
    for oz, oc in pix_peers[:-1]:
        pl.semaphore_signal(barrier, 1, device_id={"pix": oz * 2 + oc}, device_id_type=pl.DeviceIdType.MESH)

    same = lax.broadcasted_iota(jnp.int32, (nb, nb), 0) == lax.broadcasted_iota(jnp.int32, (nb, nb), 1)
    for k in range(ITERS):
        row = jnp.broadcast_to(rank_ref[k : k + 1, :], (nb, nb))
        column = jnp.sum(jnp.where(same & (row < keep_count), 1.0, 0.0), axis=1, keepdims=True)
        keep_s[k] = jnp.broadcast_to(column, (nb, TILE)).reshape(nb, 1, TILE)

    for ref in (psent, ptot, gsent, gtot):
        ref[...] = jnp.zeros_like(ref)

    copy_x0.wait()
    copy_y.wait()
    pl.semaphore_wait(barrier, 2 * nb - 1 + npx - 1)

    def remote(src, dst, send, recv, where):
        return pltpu.make_async_remote_copy(
            src_ref=src, dst_ref=dst, send_sem=send, recv_sem=recv,
            device_id=where, device_id_type=pl.DeviceIdType.MESH,
        )

    def norm_of(z):
        return jnp.sum(z * z, axis=0, keepdims=True)

    def factor(k, tile, own_norm):
        total = jnp.sum(own_norm + nrv[k % 2, tile], axis=1, keepdims=True)
        rms = jnp.sqrt(total / (CH * TILE) + EPS)
        value = keep_s[(k + ITERS - 1) % ITERS, tile] * (rms / (rms + SHRINK))
        return jnp.where(k == 0, 1.0, value)

    def norm_copies(k, to):
        return [
            remote(nst, nrv.at[k % 2, b], ns.at[i], nr.at[k % 2, b], {"freq": 1 - f, "base": other})
            for i, other in enumerate(to)
        ]

    def step(k, carry):
        par = k % 2
        rounded = z_s[...].astype(BF16)
        zrv[b] = rounded
        nst[...] = norm_of(rounded.astype(F32))
        n_sends = norm_copies(k, base_peers)
        z_sends = [
            remote(zrv.at[b], zrv.at[b], zs.at[i], zr.at[b], {"base": other})
            for i, other in enumerate(base_peers[:-1])
        ]

        @pl.when(k > 0)
        def _():
            for c in n_sends:
                c.start()

        for c in z_sends:
            c.start()

        @pl.when(k == 0)
        def _():
            copy_a.wait()

            def turn(j, carry):
                block = pl.ds(pl.multiple_of(j * TILE, TILE), TILE)
                at_s[block, :] = a_s[:, block].T
                return carry

            lax.fori_loop(0, nb, turn, 0)

        for i, dq in enumerate(reversed(outward(nq_y))):
            y0 = (yy // 2 + dq) % nq_y * 2
            firsts = [xl * ny + y0, (1 - xl) * ny + y0]
            arrive = [firsts[0], firsts[0] + 1, firsts[1], firsts[1] + 1]
            if dq == 0:
                arrive = [firsts[0] + 1 - yy % 2, firsts[1], firsts[1] + 1]
            for t in arrive:
                local_wait(zrv.at[t], zr.at[t])

            @pl.when(k > 0)
            def _():
                for t0 in firsts:
                    for t in (t0, t0 + 1):
                        local_wait(nrv.at[par, t], nr.at[par, t])

            for t0 in firsts:
                parts = []
                for t in (t0, t0 + 1):
                    tile = zrv[t].astype(F32)
                    parts.append((tile * factor(k, t, norm_of(tile))).astype(BF16))
                lhs = jnp.concatenate(parts, axis=1)
                these = pl.ds(pl.multiple_of(t0 * TILE, 2 * TILE), 2 * TILE)
                for n in range(0, rows, 256):
                    part = jnp.dot(lhs, at_s[these, n : n + 256], preferred_element_type=F32)
                    if i == 0 and t0 is firsts[0]:
                        acc[:, n : n + 256] = part
                    else:
                        acc[:, n : n + 256] += part

        half = nz // 2
        for z_ in range(nz):
            at = z_ % half, z_ // half
            pst[at] = (acc[:, TILE * z_ : TILE * z_ + TILE] - psent[at]).astype(BF16)
        p_sends = [
            remote(
                pst.at[(zz + dz) % nz % half], prv.at[par, zz, cc], ps.at[i], pr.at[par, zz, cc],
                {"pix": (zz + dz) % nz * 2 + OWNER},
            )
            for i, dz in enumerate(outward(nz))
        ]
        for c in p_sends[:-1]:
            c.start()
        psent[...] += pst[...].astype(F32)
        mine = zz % half
        near = [0]
        for d in range(1, half // 2 + 1):
            near += [d] if 2 * d == half else [d, -d]
        r_sends = [
            remote(rrv.at[mine], rrv.at[mine], rs.at[i], rr.at[mine], {"pix": (zz + d + nz) % nz * 2 + c_})
            for i, (d, c_) in enumerate((d, c_) for d in reversed(near) for c_ in (1 - OWNER, OWNER))
        ][:-1]

        @pl.when(cc != OWNER)
        def _():
            p_sends[-1].start()
            local_wait(rrv.at[mine], rr.at[mine])

        @pl.when(cc == OWNER)
        def _():
            total = ptot[...] + pst[mine].astype(F32)
            for dz in reversed(outward(nz)):
                oz = (zz + dz) % nz
                for c_ in (0, 1):
                    if (dz, c_) != (0, OWNER):
                        local_wait(prv.at[par, oz, c_], pr.at[par, oz, c_])
                        total += prv[par, oz, c_].astype(F32)
            ptot[...] = total
            for h in range(2):
                own_y = y_s[:, pl.ds(pl.multiple_of((mine + h * half) * TILE, TILE), TILE)]
                rrv[mine, h] = (own_y - total[h]).astype(BF16)
            for c in r_sends:
                c.start()

        for i, d in enumerate(near):
            q = (zz - d + nz) % half
            if d != 0:
                local_wait(rrv.at[q], rr.at[q])
            lhs = jnp.concatenate([rrv[q, 0], rrv[q, 1]], axis=1)
            low = pl.ds(pl.multiple_of(q * TILE, TILE), TILE)
            high = pl.ds(pl.multiple_of((q + half) * TILE, TILE), TILE)
            if i < len(near) - 1:
                for n in range(nb // 2):
                    cols = slice(n * 256, n * 256 + 256)
                    rhs = jnp.concatenate([a_s[low, cols], a_s[high, cols]], axis=0)
                    part = jnp.dot(lhs, rhs, preferred_element_type=F32)
                    if i == 0:
                        gacc[n] = part
                    else:
                        gacc[n] += part

        def g_copy(i, other):
            return remote(gst.at[other], grv.at[b], gs.at[i], gr.at[b], {"base": other})

        g_pairs = [((xl + dx) % 2 * ny + (yy // 2 + dq) % nq_y * 2) for dq in outward(nq_y) for dx in (1, 0)]
        g_order = []
        for t0 in g_pairs[:-1]:
            g_order += [t0, t0 + 1]
        g_order.append(g_pairs[-1] + 1 - yy % 2)
        g_sends = [g_copy(i, other) for i, other in enumerate(g_order)]

        @pl.when(k > 0)
        def _():
            for c in g_sends:
                c.wait_send()

        batch = max(len(g_pairs) // 2, 1)
        for j in range(0, len(g_pairs), batch):
            for t0 in g_pairs[j : j + batch]:
                cols = pl.ds(pl.multiple_of(t0 * TILE, 2 * TILE), 2 * TILE)
                rhs = jnp.concatenate([a_s[low, cols], a_s[high, cols]], axis=0)
                part = jnp.dot(lhs, rhs, preferred_element_type=F32)
                if len(near) > 1:
                    part += gacc[t0 // 2]
                gst[t0] = (part[:, :TILE] - gsent[t0]).astype(BF16)
                gst[t0 + 1] = (part[:, TILE:] - gsent[t0 + 1]).astype(BF16)
            for c in g_sends[2 * j : 2 * (j + batch)]:
                c.start()
        for c in z_sends + p_sends[:-1]:
            c.wait_send()

        @pl.when(k > 0)
        def _():
            for c in n_sends:
                c.wait_send()

        @pl.when(cc != OWNER)
        def _():
            p_sends[-1].wait_send()

        @pl.when(cc == OWNER)
        def _():
            for c in r_sends:
                c.wait_send()

        gsent[...] += gst[...].astype(F32)
        x = z_s[...] * factor(k, b, norm_of(zrv[b].astype(F32)))
        total = gtot[...] + gst[b].astype(F32)
        for other in reversed(base_peers[:-1]):
            local_wait(grv.at[other], gr.at[other])
            total += grv[other].astype(F32)
        gtot[...] = total
        z_s[...] = x + STRIDE * total
        return carry

    lax.fori_loop(0, ITERS, step, 0)

    for i, other in enumerate(base_peers[:-1]):
        remote(gst.at[other], grv.at[b], gs.at[i], gr.at[b], {"base": other}).wait_send()
    z = z_s[...]
    nst[...] = norm_of(z)
    (send,) = norm_copies(ITERS, [b])
    send.start()
    local_wait(nrv.at[ITERS % 2, b], nr.at[ITERS % 2, b])
    send.wait_send()
    out_ref[...] = z * factor(ITERS, b, nst[...])


def on_device(nb, npx, sensing_operator_parts, sampled_correlations, first_sky_estimate, patch_order_record):
    a = sensing_operator_parts[0]
    chans, rows = sampled_correlations.shape
    pixels = a.shape[1]
    nz = npx // 2
    dma = pltpu.SemaphoreType.DMA
    anywhere = pl.BlockSpec(memory_space=pl.ANY)
    vmem = pl.BlockSpec(memory_space=pltpu.VMEM)
    image = pl.pallas_call(
        functools.partial(kernel, nb, npx, nb * npx // 4),
        out_shape=jax.ShapeDtypeStruct((chans, TILE), F32),
        in_specs=[anywhere, anywhere, anywhere, vmem],
        out_specs=vmem,
        scratch_shapes=[
            pltpu.VMEM((rows, pixels), BF16),
            pltpu.VMEM((pixels, rows), BF16),
            pltpu.VMEM((chans, rows), F32),
            pltpu.VMEM((chans, TILE), F32),
            pltpu.VMEM((ITERS, nb, 1, TILE), F32),
            pltpu.VMEM((nb, chans, TILE), BF16),
            pltpu.VMEM((1, TILE), F32),
            pltpu.VMEM((2, nb, 1, TILE), F32),
            pltpu.VMEM((chans, rows), F32),
            pltpu.VMEM((nz // 2, 2, chans, TILE), BF16),
            pltpu.VMEM((nz // 2, 2, chans, TILE), F32),
            pltpu.VMEM((2, chans, TILE), F32),
            pltpu.VMEM((2, nz, 2, 2, chans, TILE), BF16),
            pltpu.VMEM((nz // 2, 2, chans, TILE), BF16),
            pltpu.VMEM((nb // 2, chans, 2 * TILE), F32),
            pltpu.VMEM((nb, chans, TILE), BF16),
            pltpu.VMEM((nb, chans, TILE), F32),
            pltpu.VMEM((chans, TILE), F32),
            pltpu.VMEM((nb, chans, TILE), BF16),
            dma((3,)),
            dma((nb,)), dma((nb,)),
            dma((nb,)), dma((2, nb)),
            dma((nz,)), dma((2, nz, 2)),
            dma((nz,)), dma((nz // 2,)),
            dma((nb,)), dma((nb,)),
        ],
        compiler_params=pltpu.CompilerParams(collective_id=0, has_side_effects=True),
        name="shrinkage",
    )(a, sampled_correlations, first_sky_estimate.reshape(chans, TILE), patch_order_record)
    return image.reshape(chans, 1, 1, TILE)


def solution(mesh):
    in_specs = (
        P("freq", "base", "pix"),
        P("freq", "base"),
        P("freq", "pix", "base", None),
        P(None, "pix"),
    )
    out_specs = P("freq", "pix", "base", None)
    return jax.shard_map(
        functools.partial(on_device, mesh.shape["base"], mesh.shape["pix"]),
        mesh=mesh, in_specs=in_specs, out_specs=out_specs, check_vma=False,
    )
```
